8 devices in a mesh: tp: 4 (over z, y, x), cp: 2 (over core).
Axes of the slice: x: 2, y: 2, z: 1, core: 2. Of those that a mesh axis runs over, the one named last changes fastest.
Arguments:
- x_in: bfloat16 [6, 1536, 2560], P(None, 'cp')
- positions: int32 [1536], P('cp')
- rope_cos: float32 [1536, 256], P('cp')
- rope_sin: float32 [1536, 256], P('cp')
- norm_a: bfloat16 [2560], replicated
- wq_a: bfloat16 [2560, 2048], P(None, 'tp')
- wk_a: bfloat16 [2560, 1024], P(None, 'tp')
- wv_a: bfloat16 [2560, 1024], P(None, 'tp')
- wo_a: bfloat16 [2048, 2560], P('tp')
- norm_b: bfloat16 [2560], replicated
- wq_b: bfloat16 [2560, 2048], P(None, 'tp')
- wk_b: bfloat16 [2560, 1024], P(None, 'tp')
- wv_b: bfloat16 [2560, 1024], P(None, 'tp')
- wo_b: bfloat16 [2048, 2560], P('tp')
- grad_y: bfloat16 [6, 1536, 2560], P(None, 'cp')
Outputs:
- output 1: bfloat16 [6, 1536, 2560], P(None, 'cp')
- output 2: bfloat16 [6, 1536, 2560], P(None, 'cp')
- output 3: bfloat16 [2560], P('cp')
- output 4: bfloat16 [2560, 2048], P('cp', 'tp')
- output 5: bfloat16 [2560, 1024], P('cp', 'tp')
- output 6: bfloat16 [2560, 1024], P('cp', 'tp')
- output 7: bfloat16 [2048, 2560], P(('tp', 'cp'))
- output 8: bfloat16 [2560], P('cp')
- output 9: bfloat16 [2560, 2048], P('cp', 'tp')
- output 10: bfloat16 [2560, 1024], P('cp', 'tp')
- output 11: bfloat16 [2560, 1024], P('cp', 'tp')
- output 12: bfloat16 [2048, 2560], P(('tp', 'cp'))
All inputs are finite; a program needn't handle non-finite values.
Results may differ from the reference program's by a relative error of at most 0.02.
Values are sent between devices in bfloat16 or wider.
A program may use at most 1 GiB of HBM per device.

```python
import jax
import jax.numpy as jnp
from jax import lax

BATCH = 6
SEQ_LEN = 1536
D_MODEL = 2560
Q_HEADS = 8
KV_HEADS = 4
HEAD_DIM = 256
REF_ROWS = 128

CHUNK = 2 ** 13
ROPE_BASE = 500000.0
NORM_EPS = 1e-5
QK_EPS = 1e-6
TEMP_SCALE = 0.1
NEG_BIG = -1e30


def draw_positions(key):
    key_chunk, key_shift = jax.random.split(key)
    chunk_no = jax.random.randint(key_chunk, (), 2, 6)
    shift = jax.random.randint(key_shift, (), 1, min(SEQ_LEN, CHUNK))
    return (chunk_no * CHUNK - shift + jnp.arange(SEQ_LEN)).astype(jnp.int32)


def rope_tables(positions):
    half = HEAD_DIM // 2
    inv_freq = ROPE_BASE ** (-(jnp.arange(half).astype(jnp.float32) * 2.0 / HEAD_DIM))
    angles = positions.astype(jnp.float32)[:, None] * inv_freq[None, :]
    angles = jnp.concatenate([angles, angles], axis=1)
    return jnp.cos(angles), jnp.sin(angles)


def setup_inputs(seed: int = 0) -> dict:
    keys = jax.random.split(jax.random.key(seed), 16)
    positions = draw_positions(keys[0])
    rope_cos, rope_sin = rope_tables(positions)
    q_width = Q_HEADS * HEAD_DIM
    kv_width = KV_HEADS * HEAD_DIM
    act_shape = (BATCH, SEQ_LEN, D_MODEL)

    def weight(sub_key, rows, cols):
        return (jax.random.normal(sub_key, (rows, cols), jnp.float32) * rows ** -0.5).astype(jnp.bfloat16)

    def gain(sub_key):
        return jax.random.uniform(sub_key, (D_MODEL,), jnp.float32, 0.5, 1.5).astype(jnp.bfloat16)

    return {
        'x_in': jax.random.normal(keys[1], act_shape, jnp.float32).astype(jnp.bfloat16),
        'positions': positions,
        'rope_cos': rope_cos,
        'rope_sin': rope_sin,
        'norm_a': gain(keys[3]),
        'wq_a': weight(keys[4], D_MODEL, q_width),
        'wk_a': weight(keys[5], D_MODEL, kv_width),
        'wv_a': weight(keys[6], D_MODEL, kv_width),
        'wo_a': weight(keys[7], q_width, D_MODEL),
        'norm_b': gain(keys[8]),
        'wq_b': weight(keys[9], D_MODEL, q_width),
        'wk_b': weight(keys[10], D_MODEL, kv_width),
        'wv_b': weight(keys[11], D_MODEL, kv_width),
        'wo_b': weight(keys[12], q_width, D_MODEL),
        'grad_y': jax.random.normal(keys[2], act_shape, jnp.float32).astype(jnp.bfloat16),
    }


def rms_norm(act, gamma):
    act_wide = act.astype(jnp.float32)
    inv_rms = lax.rsqrt(jnp.mean(act_wide * act_wide, axis=-1, keepdims=True) + NORM_EPS)
    return (act_wide * inv_rms * gamma.astype(jnp.float32)).astype(jnp.bfloat16)


def project(act, weight):
    rows = act.shape[0] * act.shape[1]
    flat = jnp.dot(act.reshape(rows, act.shape[2]), weight, preferred_element_type=jnp.float32)
    return flat.reshape(act.shape[0], act.shape[1], weight.shape[1]).astype(jnp.bfloat16)


def rotate(wide, cos_tab, sin_tab):
    half = HEAD_DIM // 2
    turned = jnp.concatenate([-wide[..., half:], wide[..., :half]], axis=-1)
    return wide * cos_tab[None, :, None, :] + turned * sin_tab[None, :, None, :]


def qk_prep(raw_val, cos_tab, sin_tab):
    wide = rotate(raw_val.astype(jnp.float32), cos_tab, sin_tab)
    return (wide * lax.rsqrt(jnp.mean(wide * wide, axis=-1, keepdims=True) + QK_EPS)).astype(jnp.bfloat16)


def temperature(positions):
    return jnp.log(((positions + 1) // CHUNK).astype(jnp.float32) + 1.0) * TEMP_SCALE + 1.0


def attention(queries, keys, values, positions, local):
    scale = HEAD_DIM ** -0.5
    groups = Q_HEADS // KV_HEADS
    n_blocks = SEQ_LEN // REF_ROWS

    def block_attend(q_rows, q_pos, keys_wide, vals_wide, key_pos):
        scores = jnp.einsum('bqkgd,bskd->bkgqs', q_rows.astype(jnp.float32), keys_wide) * scale
        allowed = key_pos[None, :] <= q_pos[:, None]
        if local:
            allowed = jnp.logical_and(allowed, (key_pos // CHUNK)[None, :] == (q_pos // CHUNK)[:, None])
        attn_prob = jax.nn.softmax(jnp.where(allowed, scores, NEG_BIG), axis=-1).astype(jnp.bfloat16)
        attn_out = jnp.einsum('bkgqs,bskd->bqkgd', attn_prob.astype(jnp.float32), vals_wide)
        return attn_out.astype(jnp.bfloat16)

    keys_wide = keys.astype(jnp.float32)
    vals_wide = values.astype(jnp.float32)
    attend = jax.checkpoint(block_attend)

    def one_block(block_in):
        return attend(block_in[0], block_in[1], keys_wide, vals_wide, positions)

    q_blocks = jnp.moveaxis(queries.reshape(BATCH, n_blocks, REF_ROWS, KV_HEADS, groups, HEAD_DIM), 1, 0)
    block_outs = lax.map(one_block, (q_blocks, positions.reshape(n_blocks, REF_ROWS)))
    return jnp.moveaxis(block_outs, 0, 1).reshape(BATCH, SEQ_LEN, Q_HEADS * HEAD_DIM)


def forward(x_in, positions, rope_cos, rope_sin, norm_a, wq_a, wk_a, wv_a, wo_a, norm_b, wq_b, wk_b, wv_b, wo_b):
    q_shape = (BATCH, SEQ_LEN, KV_HEADS, Q_HEADS // KV_HEADS, HEAD_DIM)
    kv_shape = (BATCH, SEQ_LEN, KV_HEADS, HEAD_DIM)
    xn_a = rms_norm(x_in, norm_a)
    query_a = qk_prep(project(xn_a, wq_a).reshape(BATCH, SEQ_LEN, Q_HEADS, HEAD_DIM), rope_cos, rope_sin).reshape(q_shape)
    key_a = qk_prep(project(xn_a, wk_a).reshape(kv_shape), rope_cos, rope_sin)
    value_a = project(xn_a, wv_a).reshape(kv_shape)
    out_a = attention(query_a, key_a, value_a, positions, True)
    h_mid = (x_in.astype(jnp.float32) + project(out_a, wo_a).astype(jnp.float32)).astype(jnp.bfloat16)
    xn_b = rms_norm(h_mid, norm_b)
    q_temp = temperature(positions)[None, :, None]
    query_b = (project(xn_b, wq_b).astype(jnp.float32) * q_temp).astype(jnp.bfloat16).reshape(q_shape)
    key_b = project(xn_b, wk_b).reshape(kv_shape)
    value_b = project(xn_b, wv_b).reshape(kv_shape)
    out_b = attention(query_b, key_b, value_b, positions, False)
    return (h_mid.astype(jnp.float32) + project(out_b, wo_b).astype(jnp.float32)).astype(jnp.bfloat16)


def reference(x_in, positions, rope_cos, rope_sin, norm_a, wq_a, wk_a, wv_a, wo_a, norm_b, wq_b, wk_b, wv_b, wo_b, grad_y):
    def layers(x_arg, gain_a, w_qa, w_ka, w_va, w_oa, gain_b, w_qb, w_kb, w_vb, w_ob):
        return forward(x_arg, positions, rope_cos, rope_sin, gain_a, w_qa, w_ka, w_va, w_oa, gain_b, w_qb, w_kb, w_vb, w_ob)

    out_y, pullback = jax.vjp(layers, x_in, norm_a, wq_a, wk_a, wv_a, wo_a, norm_b, wq_b, wk_b, wv_b, wo_b)
    grads = pullback(grad_y)
    return (out_y, grads[0], grads[1], grads[2], grads[3], grads[4], grads[5], grads[6], grads[7], grads[8], grads[9], grads[10])
```

```python
import functools

import jax
import jax.numpy as jnp
from jax import lax
from jax.experimental import pallas as pl
from jax.experimental.pallas import tpu as pltpu
from jax.sharding import PartitionSpec as P


CHUNK = 8192
NORM_EPS = 1e-5
QK_EPS = 1e-6
TEMP_SCALE = 0.1
CHUNK_BITS = 13
HEAD = 256
TILE = 384
NEG_BIG = -1e30
F32 = jnp.float32
BF16 = jnp.bfloat16


def rms_norm(act, gamma):
    act_wide = act.astype(F32)
    inv_rms = lax.rsqrt(jnp.mean(act_wide * act_wide, axis=-1, keepdims=True) + NORM_EPS)
    return (act_wide * inv_rms * gamma.astype(F32)).astype(BF16)


def norm_backward(act, gamma, grad_out):
    act_wide = act.astype(F32)
    inv_rms = lax.rsqrt(jnp.mean(act_wide * act_wide, axis=-1, keepdims=True) + NORM_EPS)
    x_hat = act_wide * inv_rms
    grad_gain = jnp.sum(grad_out * x_hat, axis=0)
    grad_hat = grad_out * gamma.astype(F32)
    grad_act = inv_rms * (grad_hat - x_hat * jnp.mean(grad_hat * x_hat, axis=-1, keepdims=True))
    return grad_act, grad_gain


def value_a11(positions):
    return jnp.log(((positions + 1) // CHUNK).astype(F32) + 1.0) * TEMP_SCALE + 1.0


def dot_f32(spec, lhs, rhs):
    return jnp.einsum(spec, lhs, rhs, preferred_element_type=F32)


def kdot(lhs, rhs, lhs_dim, rhs_dim):
    return lax.dot_general(lhs, rhs, (((lhs_dim,), (rhs_dim,)), ((), ())), preferred_element_type=F32)


def turn(wide, cos_tab, sin_tab):
    half = HEAD // 2
    turned = jnp.concatenate([-wide[:, half:], wide[:, :half]], axis=1)
    return wide * cos_tab + turned * sin_tab


def prep_kernel(q_ref, kv_ref, cos_ref, sin_ref, q_out, kv_out):
    for src, dst, count in ((q_ref, q_out, 2), (kv_ref, kv_out, 1)):
        for head in range(count):
            cols = pl.ds(head * HEAD, HEAD)
            wide = turn(src[0, :, cols].astype(F32), cos_ref[...], sin_ref[...])
            inv = lax.rsqrt(jnp.mean(wide * wide, axis=-1, keepdims=True) + QK_EPS)
            dst[0, :, cols] = (wide * inv).astype(BF16)
    kv_out[0, :, HEAD:] = kv_ref[0, :, HEAD:]


def prep_back_kernel(q_ref, kv_ref, cos_ref, sin_ref, gq_ref, gkv_ref, q_out, kv_out):
    half = HEAD // 2
    for src, grad, dst, count in ((q_ref, gq_ref, q_out, 2), (kv_ref, gkv_ref, kv_out, 1)):
        for head in range(count):
            cols = pl.ds(head * HEAD, HEAD)
            wide = turn(src[0, :, cols].astype(F32), cos_ref[...], sin_ref[...])
            inv = lax.rsqrt(jnp.mean(wide * wide, axis=-1, keepdims=True) + QK_EPS)
            hat = wide * inv
            up = grad[0, :, cols].astype(F32)
            down = inv * (up - hat * jnp.mean(up * hat, axis=-1, keepdims=True))
            side = down * sin_ref[...]
            back = jnp.concatenate([side[:, half:], -side[:, :half]], axis=1)
            dst[0, :, cols] = (down * cos_ref[...] + back).astype(BF16)
    kv_out[0, :, HEAD:] = gkv_ref[0, :, HEAD:]


def prep_call(kernel, q_val, kv_val, cos_tab, sin_tab, *grads):
    groups, rows, wide = q_val.shape
    big = pl.BlockSpec((1, TILE, wide), lambda g, i: (g, i, 0))
    tab = pl.BlockSpec((TILE, HEAD), lambda g, i: (i, 0))
    return pl.pallas_call(
        kernel,
        grid=(groups, rows // TILE),
        in_specs=[big, big, tab, tab] + [big] * len(grads),
        out_specs=[big, big],
        out_shape=[jax.ShapeDtypeStruct(q_val.shape, BF16)] * 2,
        cost_estimate=pl.CostEstimate(flops=20 * q_val.size, bytes_accessed=10 * q_val.size, transcendentals=0),
    )(q_val, kv_val, cos_tab, sin_tab, *grads)


def tile_mask(meta, tile, keys, local):
    q_at = meta[3 + tile] + lax.broadcasted_iota(jnp.int32, (1, TILE), 1)
    low = jnp.full((1, TILE), meta[6], jnp.int32)
    if local:
        start = lax.shift_left(lax.shift_right_logical(q_at + meta[7], CHUNK_BITS), CHUNK_BITS)
        low = jnp.maximum(low, start - meta[7])
    key = lax.broadcasted_iota(jnp.int32, (keys, 1), 0)
    return (key <= q_at) & (key >= low)


def pick_window(meta, tile, prev_own, cur_own, prev_sh, cur_sh):
    own = meta[tile] == 0
    return jnp.concatenate([jnp.where(own, prev_own[0], prev_sh[0]), jnp.where(own, cur_own[0], cur_sh[0])], axis=0)


def attn_kernel(local, scale, meta, q_ref, prev_own, cur_own, prev_sh, cur_sh, o_ref, stat_ref):
    tile = pl.program_id(1)
    window = pick_window(meta, tile, prev_own, cur_own, prev_sh, cur_sh)
    key = window[:, :HEAD]
    val_t = window[:, HEAD:].T
    allowed = tile_mask(meta, tile, window.shape[0], local)
    for head in range(2):
        query = q_ref[0, :, pl.ds(head * HEAD, HEAD)]
        scores = jnp.where(allowed, kdot(key, query, 1, 1) * scale, NEG_BIG)
        top = jnp.max(scores, axis=0, keepdims=True)
        prob = jnp.exp(scores - top)
        inv = 1.0 / jnp.sum(prob, axis=0, keepdims=True)
        stat_ref[0, pl.ds(head, 1), :] = top
        stat_ref[0, pl.ds(2 + head, 1), :] = inv
        out_t = kdot(val_t, (prob * inv).astype(BF16), 1, 0)
        o_ref[head] = out_t.T.astype(BF16)


def attn_back_kernel(local, scale, meta, q_ref, prev_own, cur_own, prev_sh, cur_sh, stat_ref, g_ref, tau_ref,
                     dq_ref, dprev_own, dcur_own, dprev_sh, dcur_sh, acc):
    tile = pl.program_id(1)

    @pl.when(tile == 0)
    def _():
        acc[...] = jnp.zeros_like(acc)

    window = pick_window(meta, tile, prev_own, cur_own, prev_sh, cur_sh)
    key = window[:, :HEAD]
    val = window[:, HEAD:]
    key_t = key.T
    allowed = tile_mask(meta, tile, window.shape[0], local)
    dkey = None
    for head in range(2):
        query = q_ref[0, :, pl.ds(head * HEAD, HEAD)]
        grad = g_ref[head]
        scores = jnp.where(allowed, kdot(key, query, 1, 1) * scale, NEG_BIG)
        prob = jnp.exp(scores - stat_ref[0, pl.ds(head, 1), :]) * stat_ref[0, pl.ds(2 + head, 1), :]
        dprob = kdot(val, grad, 1, 1)
        row_dot = jnp.sum(prob * dprob, axis=0, keepdims=True)
        dscore = (prob * (dprob - row_dot) * scale).astype(BF16)
        dval_h = kdot(prob.astype(BF16), grad, 1, 0)
        dkey_h = kdot(dscore, query, 1, 0)
        dkey, dval = (dkey_h, dval_h) if dkey is None else (dkey + dkey_h, dval + dval_h)
        dq_t = kdot(key_t, dscore, 1, 0) * tau_ref[...]
        dq_ref[0, :, pl.ds(head * HEAD, HEAD)] = dq_t.T.astype(BF16)
    slot = meta[tile]
    acc[slot, :, :HEAD] += dkey
    acc[slot, :, HEAD:] += dval

    @pl.when(tile == pl.num_programs(1) - 1)
    def _():
        block = acc.shape[1] // 2
        dprev_own[0] = acc[0, :block].astype(BF16)
        dcur_own[0] = acc[0, block:]
        dprev_sh[0] = acc[1, :block].astype(BF16)
        dcur_sh[0] = acc[1, block:]


def attn_specs(block):
    wide = 2 * HEAD
    q_spec = pl.BlockSpec((1, TILE, wide), lambda g, i, meta: (g, i, 0))
    w_spec = pl.BlockSpec((1, block, wide), lambda g, i, meta: (g, 0, 0))
    o_spec = pl.BlockSpec((2, TILE, HEAD), lambda g, i, meta: (0, i, g))
    s_spec = pl.BlockSpec((1, 4, TILE), lambda g, i, meta: (g, 0, i))
    return q_spec, w_spec, o_spec, s_spec


def attn_forward(local, scale, meta, q_val, wins):
    groups, rows, _ = q_val.shape
    block = wins[0].shape[1]
    q_spec, w_spec, o_spec, s_spec = attn_specs(block)
    return pl.pallas_call(
        functools.partial(attn_kernel, local, scale),
        grid_spec=pltpu.PrefetchScalarGridSpec(
            num_scalar_prefetch=1, grid=(groups, rows // TILE),
            in_specs=[q_spec] + [w_spec] * 4, out_specs=[o_spec, s_spec]),
        out_shape=[jax.ShapeDtypeStruct((2, rows, groups * HEAD), BF16), jax.ShapeDtypeStruct((groups, 4, rows), F32)],
        compiler_params=pltpu.CompilerParams(vmem_limit_bytes=56 << 20),
        cost_estimate=pl.CostEstimate(flops=8 * q_val.size * 2 * block, bytes_accessed=12 * q_val.size,
                                      transcendentals=q_val.size * 6),
        name='attn_fwd',
    )(meta, q_val, *wins)


def attn_backward(local, scale, meta, q_val, wins, stats, grad_out, tau):
    groups, rows, wide = q_val.shape
    block = wins[0].shape[1]
    q_spec, w_spec, o_spec, s_spec = attn_specs(block)
    t_spec = pl.BlockSpec((1, TILE), lambda g, i, meta: (0, i))
    half = jax.ShapeDtypeStruct(wins[0].shape, BF16)
    full = jax.ShapeDtypeStruct(wins[0].shape, F32)
    return pl.pallas_call(
        functools.partial(attn_back_kernel, local, scale),
        grid_spec=pltpu.PrefetchScalarGridSpec(
            num_scalar_prefetch=1, grid=(groups, rows // TILE),
            in_specs=[q_spec] + [w_spec] * 4 + [s_spec, o_spec, t_spec],
            out_specs=[q_spec] + [w_spec] * 4,
            scratch_shapes=[pltpu.VMEM((2, 2 * block, wide), F32)]),
        out_shape=[jax.ShapeDtypeStruct(q_val.shape, BF16), half, full, half, full],
        compiler_params=pltpu.CompilerParams(vmem_limit_bytes=60 << 20),
        cost_estimate=pl.CostEstimate(flops=20 * q_val.size * 2 * block, bytes_accessed=20 * q_val.size,
                                      transcendentals=q_val.size * 6),
        name='attn_bwd',
    )(meta, q_val, *wins, stats, grad_out, tau)


def solution(mesh):
    tp_size = mesh.shape['tp']
    row_spec = P(None, 'cp', None)
    col_spec = P(None, 'tp')
    grid_spec = P('cp', 'tp')
    out_rows = P(('tp', 'cp'), None)
    in_specs = (row_spec, P('cp'), P('cp', None), P('cp', None),
                P(None), col_spec, col_spec, col_spec, P('tp', None),
                P(None), col_spec, col_spec, col_spec, P('tp', None), row_spec)
    out_specs = (row_spec, row_spec,
                 P('cp'), grid_spec, grid_spec, grid_spec, out_rows,
                 P('cp'), grid_spec, grid_spec, grid_spec, out_rows)

    def body(x_in, positions, rope_cos, rope_sin, norm_a, wq_a, wk_a, wv_a, wo_a,
             norm_b, wq_b, wk_b, wv_b, wo_b, grad_y):
        batch, block, d_model = x_in.shape
        head_dim = rope_cos.shape[1]
        tp_rank = lax.axis_index('tp')
        cp_rank = lax.axis_index('cp')
        par = tp_rank % 2
        n_rows = batch * block // tp_size
        half = block // 2
        scale = head_dim ** -0.5
        own_at = half * par
        shared_at = block * (1 - par)
        base_shared = half * par

        def my_rows(full):
            return lax.dynamic_slice_in_dim(full.reshape(batch * block, -1), tp_rank * n_rows, n_rows, 0)

        def row_table(tab):
            shared = lax.dynamic_slice_in_dim(tab, base_shared, half, 0)
            long = jnp.concatenate([shared, tab, shared], axis=0)
            return lax.dynamic_slice_in_dim(long, half * (1 - par), n_rows, 0)

        def gather_weight(part):
            over_tp = lax.all_gather(part, 'tp', axis=0, tiled=False)
            return lax.all_gather(over_tp, 'cp', axis=0, tiled=False)

        def gather_qkv(w_q, w_k, w_v):
            return gather_weight(jnp.where(cp_rank == 0, w_q, jnp.concatenate([w_k, w_v], axis=1)))

        def gather_out(w_o):
            part = lax.dynamic_slice_in_dim(w_o, cp_rank * head_dim, head_dim, 0)
            return gather_weight(part).reshape(2, tp_size * head_dim, d_model)

        def swap(val):
            return lax.ppermute(val, 'tp', [(i, i ^ 1) for i in range(tp_size)])

        def kv_windows(key_val):
            own = lax.dynamic_slice_in_dim(key_val, own_at, block, 1)
            shared = lax.dynamic_slice_in_dim(key_val, shared_at, half, 1)
            prev_own = lax.ppermute(own, 'cp', [(0, 1)])
            other = swap(shared)
            sh_blk = lax.dynamic_slice_in_dim(jnp.concatenate([shared, other, shared], axis=1), half * par, block, 1)
            return prev_own, own, lax.ppermute(sh_blk, 'cp', [(0, 1)]), sh_blk

        def kv_windows_back(dprev_own, dcur_own, dprev_sh, dcur_sh):
            sh_blk = dcur_sh + lax.ppermute(dprev_sh, 'cp', [(1, 0)]).astype(F32)
            own = dcur_own + lax.ppermute(dprev_own, 'cp', [(1, 0)]).astype(F32)
            mine = lax.dynamic_slice_in_dim(sh_blk, half * par, half, 1)
            theirs = lax.dynamic_slice_in_dim(sh_blk, half * (1 - par), half, 1)
            mine = (mine + swap(theirs.astype(BF16)).astype(F32)).astype(BF16)
            long = jnp.concatenate([mine, own.astype(BF16), mine], axis=1)
            return lax.dynamic_slice_in_dim(long, half * (1 - par), n_rows, 1)

        def exchange(pick, place, buf):
            for k in range(tp_size):
                peer = tp_rank ^ k
                piece = pick(peer)
                if k:
                    piece = lax.ppermute(piece, 'tp', [(i, i ^ k) for i in range(tp_size)])
                buf = place(buf, piece, peer)
            return buf

        def to_groups(val):
            return exchange(lambda p: lax.dynamic_index_in_dim(val, p, 0, keepdims=False),
                            lambda buf, piece, p: lax.dynamic_update_slice_in_dim(buf, piece, p * n_rows, 0),
                            jnp.zeros((batch * block, val.shape[2]), val.dtype))

        def heads_to_groups(val):
            return exchange(lambda p: lax.dynamic_slice_in_dim(val, p * head_dim, head_dim, 2),
                            lambda buf, piece, p: lax.dynamic_update_slice_in_dim(buf, piece, p * n_rows, 1),
                            jnp.zeros((2, batch * block, head_dim), val.dtype))

        def to_all(rows):
            return lax.all_gather(rows, 'tp', axis=0, tiled=True).reshape(batch, block, d_model)

        def cp_sum(part_of):
            sent = lax.ppermute(part_of(1 - cp_rank), 'cp', [(0, 1), (1, 0)])
            return part_of(cp_rank) + sent

        def cols(val, half_no):
            return lax.dynamic_slice_in_dim(val, half_no * (d_model // 2), d_model // 2, 1)

        def head_rows(val, half_no):
            return lax.dynamic_index_in_dim(val, half_no, 0, keepdims=False)

        w_qkv_a = gather_qkv(wq_a, wk_a, wv_a)
        w_out_a = gather_out(wo_a)
        w_qkv_b = gather_qkv(wq_b, wk_b, wv_b)
        w_out_b = gather_out(wo_b)

        meta = jnp.stack([par, 0 * par, 1 - par,
                          block + half * par, block + half * (1 - par), block + half * par,
                          block * (1 - cp_rank), positions[0] - block]).astype(jnp.int32)
        cos_r = row_table(rope_cos)
        sin_r = row_table(rope_sin)
        q_temp = row_table(value_a11(positions))
        ones = jnp.ones((1, n_rows), F32)

        xn_all = rms_norm(x_in, norm_a).reshape(batch * block, d_model)
        x_rows = my_rows(x_in)
        gy_rows = my_rows(grad_y)
        xn_a = lax.dynamic_slice_in_dim(xn_all, tp_rank * n_rows, n_rows, 0)
        kv_raw = dot_f32('rd,tdh->trh', xn_a, w_qkv_a[1]).astype(BF16)
        q_raw = dot_f32('rd,tdh->trh', xn_a, w_qkv_a[0]).astype(BF16)
        query_a, kv_a = prep_call(prep_kernel, q_raw, kv_raw, cos_r, sin_r)
        wins_a = kv_windows(kv_a)
        out_a, stat_a = attn_forward(True, scale, meta, query_a, wins_a)
        attn_a = dot_f32('crh,chd->rd', out_a, w_out_a).astype(BF16)
        h_rows = (x_rows.astype(F32) + attn_a.astype(F32)).astype(BF16)

        xn_b = rms_norm(h_rows, norm_b)
        kv_b = dot_f32('rd,tdh->trh', xn_b, w_qkv_b[1]).astype(BF16)
        wins_b = kv_windows(kv_b)
        q_b = dot_f32('rd,tdh->trh', xn_b, w_qkv_b[0]).astype(BF16)
        q_b = (q_b.astype(F32) * q_temp[None, :, None]).astype(BF16)
        out_b, stat_b = attn_forward(False, scale, meta, q_b, wins_b)
        attn_b = dot_f32('crh,chd->rd', out_b, w_out_b).astype(BF16)
        y_rows = (h_rows.astype(F32) + attn_b.astype(F32)).astype(BF16)
        out_y = to_all(y_rows)
        gy_rows, _ = lax.optimization_barrier((gy_rows, y_rows))

        grad_ob = dot_f32('rd,chd->crh', gy_rows, w_out_b).astype(BF16)
        grad_q_b, *back_b = attn_backward(False, scale, meta, q_b, wins_b, stat_b, grad_ob, q_temp[None, :])
        out_b_group = heads_to_groups(out_b)
        gy_all = grad_y.reshape(batch * block, d_model)
        grad_wo_b = cp_sum(lambda half_no: dot_f32('rh,rd->hd', head_rows(out_b_group, half_no), gy_all))
        grad_kv_b = kv_windows_back(*back_b)
        parts = []
        for grad_part in (grad_q_b, grad_kv_b):
            part_b = cp_sum(lambda half_no: dot_f32('rd,trh->tdh', cols(xn_b, half_no), grad_part))
            parts.append(lax.psum_scatter(part_b.reshape(-1, 2 * head_dim), 'tp', scatter_dimension=0, tiled=True))
        grad_wq_b, grad_wkv_b = parts
        grad_xn_b = (dot_f32('trh,tdh->rd', grad_q_b, w_qkv_b[0])
                     + dot_f32('trh,tdh->rd', grad_kv_b, w_qkv_b[1])).astype(BF16)
        grad_h_norm, gain_b = norm_backward(h_rows, norm_b, grad_xn_b.astype(F32))
        grad_h = (gy_rows.astype(F32) + grad_h_norm).astype(BF16)

        grad_oa = dot_f32('rd,chd->crh', grad_h, w_out_a).astype(BF16)
        grad_q_a, *back_a = attn_backward(True, scale, meta, query_a, wins_a, stat_a, grad_oa, ones)
        part_o = cp_sum(lambda half_no: dot_f32('rh,rd->hd', head_rows(out_a, half_no), grad_h))
        grad_wo_a = lax.psum_scatter(part_o, 'tp', scatter_dimension=0, tiled=True)
        grad_kv_a = kv_windows_back(*back_a)
        grad_q_raw, grad_kv_raw = prep_call(prep_back_kernel, q_raw, kv_raw, cos_r, sin_r, grad_q_a, grad_kv_a)
        grad_xn_q = dot_f32('trh,tdh->rd', grad_q_raw, w_qkv_a[0])
        grad_xn_a = (grad_xn_q + dot_f32('trh,tdh->rd', grad_kv_raw, w_qkv_a[1])).astype(BF16)
        grad_x_norm, gain_a = norm_backward(x_rows, norm_a, grad_xn_a.astype(F32))
        gx_rows = (grad_h.astype(F32) + grad_x_norm).astype(BF16)
        grad_x = to_all(gx_rows)
        grad_q_group = to_groups(grad_q_raw)
        grad_kv_group = to_groups(grad_kv_raw)
        grad_wq_a = cp_sum(lambda half_no: dot_f32('rd,rh->dh', cols(xn_all, half_no), grad_q_group))
        grad_wkv_a = cp_sum(lambda half_no: dot_f32('rd,rh->dh', cols(xn_all, half_no), grad_kv_group))

        gains = lax.psum(jnp.stack([gain_a, gain_b]), ('tp', 'cp'))
        gains = lax.dynamic_slice_in_dim(gains, cp_rank * (d_model // 2), d_model // 2, 1).astype(BF16)
        grad_wo_b, grad_wo_a, grad_wq_a, grad_wkv_a, grad_wq_b, grad_wkv_b = (
            val.astype(BF16) for val in (grad_wo_b, grad_wo_a, grad_wq_a, grad_wkv_a, grad_wq_b, grad_wkv_b))
        return (out_y, grad_x,
                gains[0], grad_wq_a, grad_wkv_a[:, :head_dim], grad_wkv_a[:, head_dim:], grad_wo_a,
                gains[1], grad_wq_b, grad_wkv_b[:, :head_dim], grad_wkv_b[:, head_dim:], grad_wo_b)

    return jax.shard_map(body, mesh=mesh, in_specs=in_specs, out_specs=out_specs, check_vma=False)
```

```python
import functools

import jax
import jax.numpy as jnp
from jax import lax
from jax.experimental import pallas as pl
from jax.experimental.pallas import tpu as pltpu
from jax.experimental.layout import Layout, with_layout_constraint
from jax.sharding import PartitionSpec as P


CHUNK = 8192
NORM_EPS = 1e-5
QK_EPS = 1e-6
TEMP_SCALE = 0.1
CHUNK_BITS = 13
HEAD = 256
TILE = 384
NEG_BIG = -1e30
F32 = jnp.float32
BF16 = jnp.bfloat16


def rms_norm(act, gamma):
    act_wide = act.astype(F32)
    inv_rms = lax.rsqrt(jnp.mean(act_wide * act_wide, axis=-1, keepdims=True) + NORM_EPS)
    return (act_wide * inv_rms * gamma.astype(F32)).astype(BF16)


def norm_backward(act, gamma, grad_out):
    act_wide = act.astype(F32)
    inv_rms = lax.rsqrt(jnp.mean(act_wide * act_wide, axis=-1, keepdims=True) + NORM_EPS)
    x_hat = act_wide * inv_rms
    grad_gain = jnp.sum(grad_out * x_hat, axis=0)
    grad_hat = grad_out * gamma.astype(F32)
    grad_act = inv_rms * (grad_hat - x_hat * jnp.mean(grad_hat * x_hat, axis=-1, keepdims=True))
    return grad_act, grad_gain


def value_a11(positions):
    return jnp.log(((positions + 1) // CHUNK).astype(F32) + 1.0) * TEMP_SCALE + 1.0


def dot_f32(spec, lhs, rhs):
    return jnp.einsum(spec, lhs, rhs, preferred_element_type=F32)


def kdot(lhs, rhs, lhs_dim, rhs_dim):
    return lax.dot_general(lhs, rhs, (((lhs_dim,), (rhs_dim,)), ((), ())), preferred_element_type=F32)


def turn(wide, cos_tab, sin_tab):
    half = HEAD // 2
    turned = jnp.concatenate([-wide[:, half:], wide[:, :half]], axis=1)
    return wide * cos_tab + turned * sin_tab


def prep_kernel(heads, src, cos_ref, sin_ref, dst):
    for head in range(heads):
        cols = pl.ds(head * HEAD, HEAD)
        wide = turn(src[0, :, cols].astype(F32), cos_ref[...], sin_ref[...])
        inv = lax.rsqrt(jnp.mean(wide * wide, axis=-1, keepdims=True) + QK_EPS)
        dst[0, :, cols] = (wide * inv).astype(BF16)
    if heads == 1:
        dst[0, :, HEAD:] = src[0, :, HEAD:]


def prep_back_kernel(heads, src, cos_ref, sin_ref, grad, dst):
    half = HEAD // 2
    for head in range(heads):
        cols = pl.ds(head * HEAD, HEAD)
        wide = turn(src[0, :, cols].astype(F32), cos_ref[...], sin_ref[...])
        inv = lax.rsqrt(jnp.mean(wide * wide, axis=-1, keepdims=True) + QK_EPS)
        hat = wide * inv
        up = grad[0, :, cols].astype(F32)
        down = inv * (up - hat * jnp.mean(up * hat, axis=-1, keepdims=True))
        side = down * sin_ref[...]
        back = jnp.concatenate([side[:, half:], -side[:, :half]], axis=1)
        dst[0, :, cols] = (down * cos_ref[...] + back).astype(BF16)
    if heads == 1:
        dst[0, :, HEAD:] = grad[0, :, HEAD:]


def prep_call(kernel, heads, val, cos_tab, sin_tab, *grads):
    groups, rows, wide = val.shape
    big = pl.BlockSpec((1, TILE, wide), lambda i, g: (g, i, 0))
    tab = pl.BlockSpec((TILE, HEAD), lambda i, g: (i, 0))
    return pl.pallas_call(
        functools.partial(kernel, heads),
        grid=(rows // TILE, groups),
        in_specs=[big, tab, tab] + [big] * len(grads),
        out_specs=big,
        out_shape=jax.ShapeDtypeStruct(val.shape, BF16),
        cost_estimate=pl.CostEstimate(flops=1000 * val.size, bytes_accessed=6 * val.size, transcendentals=0),
    )(val, cos_tab, sin_tab, *grads)


def tile_mask(meta, keys, local):
    q_at = meta[1] + pl.program_id(1) * TILE + lax.broadcasted_iota(jnp.int32, (1, TILE), 1)
    low = jnp.full((1, TILE), meta[2], jnp.int32)
    if local:
        start = lax.shift_left(lax.shift_right_logical(q_at + meta[3], CHUNK_BITS), CHUNK_BITS)
        low = jnp.maximum(low, start - meta[3])
    key = lax.broadcasted_iota(jnp.int32, (keys, 1), 0)
    return (key <= q_at) & (key >= low)


def attn_kernel(local, scale, meta, q_ref, prev, cur, *rest):
    o_ref, stat_ref = rest[-2:]
    window = jnp.concatenate([prev[0], cur[0]], axis=0)
    key = window[:, :HEAD]
    val_t = window[:, HEAD:].T
    allowed = tile_mask(meta, window.shape[0], local)
    for head in range(2):
        query = q_ref[0, :, pl.ds(head * HEAD, HEAD)]
        scores = jnp.where(allowed, kdot(key, query, 1, 1) * scale, NEG_BIG)
        top = jnp.max(scores, axis=0, keepdims=True)
        prob = jnp.exp(scores - top)
        inv = 1.0 / jnp.sum(prob, axis=0, keepdims=True)
        stat_ref[0, pl.ds(head, 1), :] = top
        stat_ref[0, pl.ds(2 + head, 1), :] = inv
        out_t = kdot(val_t, (prob * inv).astype(BF16), 1, 0)
        o_ref[head] = out_t.T.astype(BF16)


def attn_back_kernel(local, scale, meta, q_ref, prev, cur, stat_ref, g_ref, tau_ref, *rest):
    dq_ref, dprev, dcur, acc = rest[-4:]
    tile = pl.program_id(1)

    @pl.when(tile == 0)
    def _():
        acc[...] = jnp.zeros_like(acc)

    window = jnp.concatenate([prev[0], cur[0]], axis=0)
    key = window[:, :HEAD]
    val = window[:, HEAD:]
    key_t = key.T
    allowed = tile_mask(meta, window.shape[0], local)
    dkey = None
    for head in range(2):
        query = q_ref[0, :, pl.ds(head * HEAD, HEAD)]
        grad = g_ref[head]
        scores = jnp.where(allowed, kdot(key, query, 1, 1) * scale, NEG_BIG)
        prob = jnp.exp(scores - stat_ref[0, pl.ds(head, 1), :]) * stat_ref[0, pl.ds(2 + head, 1), :]
        dprob = kdot(val, grad, 1, 1)
        row_dot = jnp.sum(prob * dprob, axis=0, keepdims=True)
        dscore = (prob * (dprob - row_dot) * scale).astype(BF16)
        dval_h = kdot(prob.astype(BF16), grad, 1, 0)
        dkey_h = kdot(dscore, query, 1, 0)
        dkey, dval = (dkey_h, dval_h) if dkey is None else (dkey + dkey_h, dval + dval_h)
        dq_t = kdot(key_t, dscore, 1, 0) * tau_ref[...]
        dq_ref[0, :, pl.ds(head * HEAD, HEAD)] = dq_t.T.astype(BF16)
    acc[:, :HEAD] += dkey
    acc[:, HEAD:] += dval

    @pl.when(tile == pl.num_programs(1) - 1)
    def _():
        block = acc.shape[0] // 2
        dprev[0] = acc[:block].astype(BF16)
        dcur[0] = acc[block:]


def attn_specs(block):
    wide = 2 * HEAD
    q_spec = pl.BlockSpec((1, TILE, wide), lambda g, i, meta: (g, meta[0] + i, 0))
    w_spec = pl.BlockSpec((1, block, wide), lambda g, i, meta: (g, 0, 0))
    o_spec = pl.BlockSpec((2, TILE, HEAD), lambda g, i, meta: (0, meta[0] + i, g))
    s_spec = pl.BlockSpec((1, 4, TILE), lambda g, i, meta: (g, 0, i))
    t_spec = pl.BlockSpec((1, TILE), lambda g, i, meta: (0, meta[0] + i))
    return q_spec, w_spec, o_spec, s_spec, t_spec


def attn_forward(local, scale, meta, tiles, q_val, window, into=()):
    groups, rows, wide = q_val.shape
    block = window[0].shape[1]
    q_spec, w_spec, o_spec, s_spec, _ = attn_specs(block)
    work = groups * tiles * TILE * wide
    return pl.pallas_call(
        functools.partial(attn_kernel, local, scale),
        grid_spec=pltpu.PrefetchScalarGridSpec(
            num_scalar_prefetch=1, grid=(groups, tiles),
            in_specs=[q_spec, w_spec, w_spec] + [pl.BlockSpec(memory_space=pl.ANY)] * len(into),
            out_specs=[o_spec, s_spec]),
        out_shape=[jax.ShapeDtypeStruct((2, rows, groups * HEAD), BF16),
                   jax.ShapeDtypeStruct((groups, 4, tiles * TILE), F32)],
        input_output_aliases={4: 0} if into else {},
        compiler_params=pltpu.CompilerParams(vmem_limit_bytes=56 << 20),
        cost_estimate=pl.CostEstimate(flops=8 * work * 2 * block, bytes_accessed=12 * work, transcendentals=work * 6),
        name='attn_fwd',
    )(meta, q_val, *window, *into)


def attn_backward(local, scale, meta, tiles, q_val, window, stats, grad_out, tau, into=()):
    groups, _, wide = q_val.shape
    block = window[0].shape[1]
    q_spec, w_spec, o_spec, s_spec, t_spec = attn_specs(block)
    work = groups * tiles * TILE * wide
    return pl.pallas_call(
        functools.partial(attn_back_kernel, local, scale),
        grid_spec=pltpu.PrefetchScalarGridSpec(
            num_scalar_prefetch=1, grid=(groups, tiles),
            in_specs=[q_spec, w_spec, w_spec, s_spec, o_spec, t_spec] + [pl.BlockSpec(memory_space=pl.ANY)] * len(into),
            out_specs=[q_spec, w_spec, w_spec],
            scratch_shapes=[pltpu.VMEM((2 * block, wide), F32)]),
        out_shape=[jax.ShapeDtypeStruct(q_val.shape, BF16), jax.ShapeDtypeStruct(window[0].shape, BF16),
                   jax.ShapeDtypeStruct(window[0].shape, F32)],
        input_output_aliases={7: 0} if into else {},
        compiler_params=pltpu.CompilerParams(vmem_limit_bytes=60 << 20),
        cost_estimate=pl.CostEstimate(flops=20 * work * 2 * block, bytes_accessed=20 * work, transcendentals=work * 6),
        name='attn_bwd',
    )(meta, q_val, *window, stats, grad_out, tau, *into)


def solution(mesh):
    tp_size = mesh.shape['tp']
    row_spec = P(None, 'cp', None)
    col_spec = P(None, 'tp')
    grid_spec = P('cp', 'tp')
    out_rows = P(('tp', 'cp'), None)
    in_specs = (row_spec, P('cp'), P('cp', None), P('cp', None),
                P(None), col_spec, col_spec, col_spec, P('tp', None),
                P(None), col_spec, col_spec, col_spec, P('tp', None), row_spec)
    out_specs = (row_spec, row_spec,
                 P('cp'), grid_spec, grid_spec, grid_spec, out_rows,
                 P('cp'), grid_spec, grid_spec, grid_spec, out_rows)

    def body(x_in, positions, rope_cos, rope_sin, norm_a, wq_a, wk_a, wv_a, wo_a,
             norm_b, wq_b, wk_b, wv_b, wo_b, grad_y):
        batch, block, d_model = x_in.shape
        head_dim = rope_cos.shape[1]
        tp_rank = lax.axis_index('tp')
        cp_rank = lax.axis_index('cp')
        par = tp_rank % 2
        n_rows = batch * block // tp_size
        half = block // 2
        scale = head_dim ** -0.5
        own_at = half * par
        shared_at = block * (1 - par)
        base_shared = half * par

        def my_rows(full):
            return lax.dynamic_slice_in_dim(full.reshape(batch * block, -1), tp_rank * n_rows, n_rows, 0)

        def row_table(tab):
            shared = lax.dynamic_slice_in_dim(tab, base_shared, half, 0)
            long = jnp.concatenate([shared, tab, shared], axis=0)
            return lax.dynamic_slice_in_dim(long, half * (1 - par), n_rows, 0)

        def gather_weight(part):
            over_tp = lax.all_gather(part, 'tp', axis=0, tiled=False)
            return lax.all_gather(over_tp, 'cp', axis=0, tiled=False)

        def gather_qkv(w_q, w_k, w_v):
            return gather_weight(jnp.where(cp_rank == 0, w_q, jnp.concatenate([w_k, w_v], axis=1)))

        def gather_out(w_o):
            part = lax.dynamic_slice_in_dim(w_o, cp_rank * head_dim, head_dim, 0)
            return gather_weight(part).reshape(2, tp_size * head_dim, d_model)

        def swap(val):
            return lax.ppermute(val, 'tp', [(i, i ^ 1) for i in range(tp_size)])

        def attention(local, key_val, make_query):
            own = lax.dynamic_slice_in_dim(key_val, own_at, block, 1)
            shared = lax.dynamic_slice_in_dim(key_val, shared_at, half, 1)
            other = swap(shared)
            win_own = (lax.ppermute(own, 'cp', [(0, 1)]), own)
            query = make_query()
            out, stat_own = attn_forward(local, scale, meta_own, 2, query, win_own)
            sh_blk = lax.dynamic_slice_in_dim(jnp.concatenate([shared, other, shared], axis=1), half * par, block, 1)
            win_sh = (lax.ppermute(sh_blk, 'cp', [(0, 1)]), sh_blk)
            out, stat_sh = attn_forward(local, scale, meta_sh, 1, query, win_sh, (out,))
            return out, (query, win_own, win_sh, stat_own, stat_sh)

        def attention_back(local, saved, grad_out, tau):
            query, win_own, win_sh, stat_own, stat_sh = saved
            grad_q, dprev, dcur = attn_backward(local, scale, meta_sh, 1, query, win_sh, stat_sh, grad_out, tau)
            sh_blk = dcur + lax.ppermute(dprev, 'cp', [(1, 0)]).astype(F32)
            mine = lax.dynamic_slice_in_dim(sh_blk, half * par, half, 1)
            theirs = lax.dynamic_slice_in_dim(sh_blk, half * (1 - par), half, 1).astype(BF16)
            theirs = swap(theirs)
            grad_q, dprev, dcur = attn_backward(local, scale, meta_own, 2, query, win_own, stat_own, grad_out, tau,
                                                (grad_q,))
            mine = (mine + theirs.astype(F32)).astype(BF16)
            own = (dcur + lax.ppermute(dprev, 'cp', [(1, 0)]).astype(F32)).astype(BF16)
            long = jnp.concatenate([mine, own, mine], axis=1)
            return grad_q, lax.dynamic_slice_in_dim(long, half * (1 - par), n_rows, 1)

        def exchange(pick, place, buf):
            for k in range(tp_size):
                peer = tp_rank ^ k
                piece = pick(peer)
                if k:
                    piece = lax.ppermute(piece, 'tp', [(i, i ^ k) for i in range(tp_size)])
                buf = place(buf, piece, peer)
            return buf

        def to_groups(val):
            return exchange(lambda p: lax.dynamic_index_in_dim(val, p, 0, keepdims=False),
                            lambda buf, piece, p: lax.dynamic_update_slice_in_dim(buf, piece, p * n_rows, 0),
                            jnp.zeros((batch * block, val.shape[2]), val.dtype))

        def heads_to_groups(val):
            return exchange(lambda p: lax.dynamic_slice_in_dim(val, p * head_dim, head_dim, 2),
                            lambda buf, piece, p: lax.dynamic_update_slice_in_dim(buf, piece, p * n_rows, 1),
                            jnp.zeros((2, batch * block, head_dim), val.dtype))

        def to_all(rows):
            own = lax.dynamic_slice_in_dim(rows, own_at, block, 0)
            shared = lax.dynamic_slice_in_dim(rows, shared_at, half, 0)
            shared = lax.all_gather(shared, 'tp', axis=0, tiled=True)
            own = lax.all_gather(own, 'tp', axis=0, tiled=True)
            pieces = []
            for chip in range(tp_size):
                pair = [own[block * chip:block * (chip + 1)], shared[half * chip:half * (chip + 1)]]
                pieces += pair[::-1] if chip % 2 else pair
            return jnp.concatenate(pieces, axis=0).reshape(batch, block, d_model)

        def cp_sum(part_of):
            sent = lax.ppermute(part_of(1 - cp_rank), 'cp', [(0, 1), (1, 0)])
            return part_of(cp_rank) + sent

        def cols(val, half_no):
            return lax.dynamic_slice_in_dim(val, half_no * (d_model // 2), d_model // 2, 1)

        def head_rows(val, half_no):
            return lax.dynamic_index_in_dim(val, half_no, 0, keepdims=False)

        w_qkv_a = gather_qkv(wq_a, wk_a, wv_a)
        w_out_a = gather_out(wo_a)
        w_qkv_b = gather_qkv(wq_b, wk_b, wv_b)
        w_out_b = gather_out(wo_b)

        key_at = [block * (1 - cp_rank), positions[0] - block]
        meta_own = jnp.stack([par, block + 0 * par] + key_at).astype(jnp.int32)
        meta_sh = jnp.stack([2 * (1 - par), block + half * par] + key_at).astype(jnp.int32)
        cos_r = row_table(rope_cos)
        sin_r = row_table(rope_sin)
        q_temp = row_table(value_a11(positions))
        ones = jnp.ones((1, n_rows), F32)

        xn_all = rms_norm(x_in, norm_a).reshape(batch * block, d_model)
        xn_a = lax.dynamic_slice_in_dim(xn_all, tp_rank * n_rows, n_rows, 0)
        x_rows = my_rows(x_in)
        gy_rows = my_rows(grad_y)
        kv_raw = dot_f32('rd,tdh->trh', xn_a, w_qkv_a[1]).astype(BF16)
        kv_a = prep_call(prep_kernel, 1, kv_raw, cos_r, sin_r)

        def query_a():
            raw = dot_f32('rd,tdh->trh', xn_a, w_qkv_a[0]).astype(BF16)
            q_raws.append(raw)
            return prep_call(prep_kernel, 2, raw, cos_r, sin_r)

        q_raws = []
        out_a, saved_a = attention(True, kv_a, query_a)
        q_raw = q_raws[0]
        attn_a = dot_f32('crh,chd->rd', out_a, w_out_a).astype(BF16)
        h_rows = (x_rows.astype(F32) + attn_a.astype(F32)).astype(BF16)

        xn_b = rms_norm(h_rows, norm_b)
        kv_b = dot_f32('rd,tdh->trh', xn_b, w_qkv_b[1]).astype(BF16)

        def query_b():
            raw = dot_f32('rd,tdh->trh', xn_b, w_qkv_b[0]).astype(BF16)
            return (raw.astype(F32) * q_temp[None, :, None]).astype(BF16)

        out_b, saved_b = attention(False, kv_b, query_b)
        attn_b = dot_f32('crh,chd->rd', out_b, w_out_b).astype(BF16)
        y_rows = (h_rows.astype(F32) + attn_b.astype(F32)).astype(BF16)
        out_y = to_all(y_rows)
        gy_rows, _ = lax.optimization_barrier((gy_rows, y_rows))

        grad_ob = dot_f32('rd,chd->crh', gy_rows, w_out_b).astype(BF16)
        grad_q_b, grad_kv_b = attention_back(False, saved_b, grad_ob, q_temp[None, :])
        out_b_group = heads_to_groups(out_b)
        gy_all = grad_y.reshape(batch * block, d_model)
        grad_wo_b = cp_sum(lambda half_no: dot_f32('rh,rd->hd', head_rows(out_b_group, half_no), gy_all))
        parts = []
        for grad_part in (grad_q_b, grad_kv_b):
            part_b = cp_sum(lambda half_no: dot_f32('rd,trh->thd', cols(xn_b, half_no), grad_part))
            part_b = with_layout_constraint(part_b.reshape(-1, d_model // 2), Layout((0, 1)))
            part_b = lax.psum_scatter(part_b, 'tp', scatter_dimension=0, tiled=True)
            part_b = with_layout_constraint(part_b, Layout((0, 1)))
            parts.append(part_b.T)
        grad_wq_b, grad_wkv_b = parts
        grad_xn_b = (dot_f32('trh,tdh->rd', grad_q_b, w_qkv_b[0])
                     + dot_f32('trh,tdh->rd', grad_kv_b, w_qkv_b[1])).astype(BF16)
        grad_h_norm, gain_b = norm_backward(h_rows, norm_b, grad_xn_b.astype(F32))
        grad_h = (gy_rows.astype(F32) + grad_h_norm).astype(BF16)

        grad_oa = dot_f32('rd,chd->crh', grad_h, w_out_a).astype(BF16)
        grad_q_a, grad_kv_a = attention_back(True, saved_a, grad_oa, ones)
        part_o = cp_sum(lambda half_no: dot_f32('rh,rd->hd', head_rows(out_a, half_no), grad_h))
        grad_wo_a = lax.psum_scatter(part_o, 'tp', scatter_dimension=0, tiled=True)
        grad_q_raw = prep_call(prep_back_kernel, 2, q_raw, cos_r, sin_r, grad_q_a)
        grad_kv_raw = prep_call(prep_back_kernel, 1, kv_raw, cos_r, sin_r, grad_kv_a)
        grad_xn_q = dot_f32('trh,tdh->rd', grad_q_raw, w_qkv_a[0])
        grad_xn_a = (grad_xn_q + dot_f32('trh,tdh->rd', grad_kv_raw, w_qkv_a[1])).astype(BF16)
        grad_x_norm, gain_a = norm_backward(x_rows, norm_a, grad_xn_a.astype(F32))
        gx_rows = (grad_h.astype(F32) + grad_x_norm).astype(BF16)
        grad_x = to_all(gx_rows)
        grad_q_group = to_groups(grad_q_raw)
        grad_kv_group = to_groups(grad_kv_raw)
        grad_wq_a = cp_sum(lambda half_no: dot_f32('rd,rh->dh', cols(xn_all, half_no), grad_q_group))
        grad_wkv_a = cp_sum(lambda half_no: dot_f32('rd,rh->dh', cols(xn_all, half_no), grad_kv_group))

        gains = lax.psum(jnp.stack([gain_a, gain_b]), ('tp', 'cp'))
        gains = lax.dynamic_slice_in_dim(gains, cp_rank * (d_model // 2), d_model // 2, 1).astype(BF16)
        grad_wo_b, grad_wo_a, grad_wq_a, grad_wkv_a, grad_wq_b, grad_wkv_b = (
            val.astype(BF16) for val in (grad_wo_b, grad_wo_a, grad_wq_a, grad_wkv_a, grad_wq_b, grad_wkv_b))
        return (out_y, grad_x,
                gains[0], grad_wq_a, grad_wkv_a[:, :head_dim], grad_wkv_a[:, head_dim:], grad_wo_a,
                gains[1], grad_wq_b, grad_wkv_b[:, :head_dim], grad_wkv_b[:, head_dim:], grad_wo_b)

    return jax.shard_map(body, mesh=mesh, in_specs=in_specs, out_specs=out_specs, check_vma=False)
```

```python
import functools

import jax
import jax.numpy as jnp
from jax import lax
from jax.experimental import pallas as pl
from jax.experimental.pallas import tpu as pltpu
from jax.experimental.layout import Layout, with_layout_constraint
from jax.sharding import PartitionSpec as P


CHUNK = 8192
NORM_EPS = 1e-5
QK_EPS = 1e-6
TEMP_SCALE = 0.1
CHUNK_BITS = 13
HEAD = 256
TILE = 384
NEG_BIG = -1e30
F32 = jnp.float32
BF16 = jnp.bfloat16


def rms_norm(act, gamma):
    act_wide = act.astype(F32)
    inv_rms = lax.rsqrt(jnp.mean(act_wide * act_wide, axis=-1, keepdims=True) + NORM_EPS)
    return (act_wide * inv_rms * gamma.astype(F32)).astype(BF16)


def norm_backward(act, gamma, grad_out):
    act_wide = act.astype(F32)
    inv_rms = lax.rsqrt(jnp.mean(act_wide * act_wide, axis=-1, keepdims=True) + NORM_EPS)
    x_hat = act_wide * inv_rms
    grad_gain = jnp.sum(grad_out * x_hat, axis=0)
    grad_hat = grad_out * gamma.astype(F32)
    grad_act = inv_rms * (grad_hat - x_hat * jnp.mean(grad_hat * x_hat, axis=-1, keepdims=True))
    return grad_act, grad_gain


def value_a11(positions):
    return jnp.log(((positions + 1) // CHUNK).astype(F32) + 1.0) * TEMP_SCALE + 1.0


def dot_f32(spec, lhs, rhs):
    return jnp.einsum(spec, lhs, rhs, preferred_element_type=F32)


def kdot(lhs, rhs, lhs_dim, rhs_dim):
    return lax.dot_general(lhs, rhs, (((lhs_dim,), (rhs_dim,)), ((), ())), preferred_element_type=F32)


def turn(wide, cos_tab, sin_tab):
    half = HEAD // 2
    turned = jnp.concatenate([-wide[:, half:], wide[:, :half]], axis=1)
    return wide * cos_tab + turned * sin_tab


def prep_kernel(heads, src, cos_ref, sin_ref, dst):
    for head in range(heads):
        cols = pl.ds(head * HEAD, HEAD)
        wide = turn(src[0, :, cols].astype(F32), cos_ref[...], sin_ref[...])
        inv = lax.rsqrt(jnp.mean(wide * wide, axis=-1, keepdims=True) + QK_EPS)
        dst[0, :, cols] = (wide * inv).astype(BF16)
    if heads == 1:
        dst[0, :, HEAD:] = src[0, :, HEAD:]


def prep_back_kernel(heads, src, cos_ref, sin_ref, grad, dst):
    half = HEAD // 2
    for head in range(heads):
        cols = pl.ds(head * HEAD, HEAD)
        wide = turn(src[0, :, cols].astype(F32), cos_ref[...], sin_ref[...])
        inv = lax.rsqrt(jnp.mean(wide * wide, axis=-1, keepdims=True) + QK_EPS)
        hat = wide * inv
        up = grad[0, :, cols].astype(F32)
        down = inv * (up - hat * jnp.mean(up * hat, axis=-1, keepdims=True))
        side = down * sin_ref[...]
        back = jnp.concatenate([side[:, half:], -side[:, :half]], axis=1)
        dst[0, :, cols] = (down * cos_ref[...] + back).astype(BF16)
    if heads == 1:
        dst[0, :, HEAD:] = grad[0, :, HEAD:]


def prep_call(kernel, heads, val, cos_tab, sin_tab, *grads):
    groups, rows, wide = val.shape
    big = pl.BlockSpec((1, TILE, wide), lambda i, g: (g, i, 0))
    tab = pl.BlockSpec((TILE, HEAD), lambda i, g: (i, 0))
    return pl.pallas_call(
        functools.partial(kernel, heads),
        grid=(rows // TILE, groups),
        in_specs=[big, tab, tab] + [big] * len(grads),
        out_specs=big,
        out_shape=jax.ShapeDtypeStruct(val.shape, BF16),
        cost_estimate=pl.CostEstimate(flops=1000 * val.size, bytes_accessed=6 * val.size, transcendentals=0),
    )(val, cos_tab, sin_tab, *grads)


def tile_mask(meta, keys, local):
    q_at = meta[1] + pl.program_id(1) * TILE + lax.broadcasted_iota(jnp.int32, (1, TILE), 1)
    low = jnp.full((1, TILE), meta[2], jnp.int32)
    if local:
        start = lax.shift_left(lax.shift_right_logical(q_at + meta[3], CHUNK_BITS), CHUNK_BITS)
        low = jnp.maximum(low, start - meta[3])
    key = lax.broadcasted_iota(jnp.int32, (keys, 1), 0)
    return (key <= q_at) & (key >= low)


def attn_kernel(local, scale, meta, q_ref, prev, cur, *rest):
    o_ref, stat_ref = rest[-2:]
    window = jnp.concatenate([prev[0], cur[0]], axis=0)
    key = window[:, :HEAD]
    val_t = window[:, HEAD:].T
    allowed = tile_mask(meta, window.shape[0], local)
    for head in range(2):
        query = q_ref[0, :, pl.ds(head * HEAD, HEAD)]
        scores = jnp.where(allowed, kdot(key, query, 1, 1) * scale, NEG_BIG)
        top = jnp.max(scores, axis=0, keepdims=True)
        prob = jnp.exp(scores - top)
        inv = 1.0 / jnp.sum(prob, axis=0, keepdims=True)
        stat_ref[0, pl.ds(head, 1), :] = top
        stat_ref[0, pl.ds(2 + head, 1), :] = inv
        out_t = kdot(val_t, (prob * inv).astype(BF16), 1, 0)
        o_ref[head] = out_t.T.astype(BF16)


def attn_back_kernel(local, scale, meta, q_ref, prev, cur, stat_ref, g_ref, tau_ref, *rest):
    dq_ref, dprev, dcur, acc = rest[-4:]
    tile = pl.program_id(1)

    @pl.when(tile == 0)
    def _():
        acc[...] = jnp.zeros_like(acc)

    window = jnp.concatenate([prev[0], cur[0]], axis=0)
    key = window[:, :HEAD]
    val = window[:, HEAD:]
    key_t = key.T
    allowed = tile_mask(meta, window.shape[0], local)
    dkey = None
    for head in range(2):
        query = q_ref[0, :, pl.ds(head * HEAD, HEAD)]
        grad = g_ref[head]
        scores = jnp.where(allowed, kdot(key, query, 1, 1) * scale, NEG_BIG)
        prob = jnp.exp(scores - stat_ref[0, pl.ds(head, 1), :]) * stat_ref[0, pl.ds(2 + head, 1), :]
        dprob = kdot(val, grad, 1, 1)
        row_dot = jnp.sum(prob * dprob, axis=0, keepdims=True)
        dscore = (prob * (dprob - row_dot) * scale).astype(BF16)
        dval_h = kdot(prob.astype(BF16), grad, 1, 0)
        dkey_h = kdot(dscore, query, 1, 0)
        dkey, dval = (dkey_h, dval_h) if dkey is None else (dkey + dkey_h, dval + dval_h)
        dq_t = kdot(key_t, dscore, 1, 0) * tau_ref[...]
        dq_ref[0, :, pl.ds(head * HEAD, HEAD)] = dq_t.T.astype(BF16)
    acc[:, :HEAD] += dkey
    acc[:, HEAD:] += dval

    @pl.when(tile == pl.num_programs(1) - 1)
    def _():
        block = acc.shape[0] // 2
        dprev[0] = acc[:block].astype(BF16)
        dcur[0] = acc[block:]


def attn_specs(block):
    wide = 2 * HEAD
    q_spec = pl.BlockSpec((1, TILE, wide), lambda g, i, meta: (g, meta[0] + i, 0))
    w_spec = pl.BlockSpec((1, block, wide), lambda g, i, meta: (g, 0, 0))
    o_spec = pl.BlockSpec((2, TILE, HEAD), lambda g, i, meta: (0, meta[0] + i, g))
    s_spec = pl.BlockSpec((1, 4, TILE), lambda g, i, meta: (g, 0, i))
    t_spec = pl.BlockSpec((1, TILE), lambda g, i, meta: (0, meta[0] + i))
    return q_spec, w_spec, o_spec, s_spec, t_spec


def attn_forward(local, scale, meta, tiles, q_val, window, into=()):
    groups, rows, wide = q_val.shape
    block = window[0].shape[1]
    q_spec, w_spec, o_spec, s_spec, _ = attn_specs(block)
    work = groups * tiles * TILE * wide
    return pl.pallas_call(
        functools.partial(attn_kernel, local, scale),
        grid_spec=pltpu.PrefetchScalarGridSpec(
            num_scalar_prefetch=1, grid=(groups, tiles),
            in_specs=[q_spec, w_spec, w_spec] + [pl.BlockSpec(memory_space=pl.ANY)] * len(into),
            out_specs=[o_spec, s_spec]),
        out_shape=[jax.ShapeDtypeStruct((2, rows, groups * HEAD), BF16),
                   jax.ShapeDtypeStruct((groups, 4, tiles * TILE), F32)],
        input_output_aliases={4: 0} if into else {},
        compiler_params=pltpu.CompilerParams(vmem_limit_bytes=56 << 20),
        cost_estimate=pl.CostEstimate(flops=8 * work * 2 * block, bytes_accessed=12 * work, transcendentals=work * 6),
        name='attn_fwd',
    )(meta, q_val, *window, *into)


def attn_backward(local, scale, meta, tiles, q_val, window, stats, grad_out, tau, into=()):
    groups, _, wide = q_val.shape
    block = window[0].shape[1]
    q_spec, w_spec, o_spec, s_spec, t_spec = attn_specs(block)
    work = groups * tiles * TILE * wide
    return pl.pallas_call(
        functools.partial(attn_back_kernel, local, scale),
        grid_spec=pltpu.PrefetchScalarGridSpec(
            num_scalar_prefetch=1, grid=(groups, tiles),
            in_specs=[q_spec, w_spec, w_spec, s_spec, o_spec, t_spec] + [pl.BlockSpec(memory_space=pl.ANY)] * len(into),
            out_specs=[q_spec, w_spec, w_spec],
            scratch_shapes=[pltpu.VMEM((2 * block, wide), F32)]),
        out_shape=[jax.ShapeDtypeStruct(q_val.shape, BF16), jax.ShapeDtypeStruct(window[0].shape, BF16),
                   jax.ShapeDtypeStruct(window[0].shape, F32)],
        input_output_aliases={7: 0} if into else {},
        compiler_params=pltpu.CompilerParams(vmem_limit_bytes=60 << 20),
        cost_estimate=pl.CostEstimate(flops=20 * work * 2 * block, bytes_accessed=20 * work, transcendentals=work * 6),
        name='attn_bwd',
    )(meta, q_val, *window, stats, grad_out, tau, *into)


def solution(mesh):
    tp_size = mesh.shape['tp']
    row_spec = P(None, 'cp', None)
    col_spec = P(None, 'tp')
    grid_spec = P('cp', 'tp')
    out_rows = P(('tp', 'cp'), None)
    in_specs = (row_spec, P('cp'), P('cp', None), P('cp', None),
                P(None), col_spec, col_spec, col_spec, P('tp', None),
                P(None), col_spec, col_spec, col_spec, P('tp', None), row_spec)
    out_specs = (row_spec, row_spec,
                 P('cp'), grid_spec, grid_spec, grid_spec, out_rows,
                 P('cp'), grid_spec, grid_spec, grid_spec, out_rows)

    def body(x_in, positions, rope_cos, rope_sin, norm_a, wq_a, wk_a, wv_a, wo_a,
             norm_b, wq_b, wk_b, wv_b, wo_b, grad_y):
        batch, block, d_model = x_in.shape
        head_dim = rope_cos.shape[1]
        tp_rank = lax.axis_index('tp')
        cp_rank = lax.axis_index('cp')
        par = tp_rank % 2
        n_rows = batch * block // tp_size
        half = block // 2
        scale = head_dim ** -0.5
        own_at = half * par
        shared_at = block * (1 - par)
        base_shared = half * par

        def my_rows(full):
            return lax.dynamic_slice_in_dim(full.reshape(batch * block, -1), tp_rank * n_rows, n_rows, 0)

        def row_table(tab):
            shared = lax.dynamic_slice_in_dim(tab, base_shared, half, 0)
            long = jnp.concatenate([shared, tab, shared], axis=0)
            return lax.dynamic_slice_in_dim(long, half * (1 - par), n_rows, 0)

        def gather_weight(part):
            over_tp = lax.all_gather(part, 'tp', axis=0, tiled=False)
            other = lax.ppermute(over_tp, 'cp', [(0, 1), (1, 0)])
            return jnp.where(cp_rank == 0, over_tp, other), jnp.where(cp_rank == 0, other, over_tp)

        def gather_qkv(w_q, w_k, w_v):
            return gather_weight(jnp.where(cp_rank == 0, w_q, jnp.concatenate([w_k, w_v], axis=1)))

        def gather_out(w_o):
            part = lax.dynamic_slice_in_dim(w_o, cp_rank * head_dim, head_dim, 0)
            return jnp.stack(gather_weight(part)).reshape(2, tp_size * head_dim, d_model)

        def swap(val):
            return lax.ppermute(val, 'tp', [(i, i ^ 1) for i in range(tp_size)])

        def attention(local, key_val, make_query):
            own = lax.dynamic_slice_in_dim(key_val, own_at, block, 1)
            shared = lax.dynamic_slice_in_dim(key_val, shared_at, half, 1)
            other = swap(shared)
            win_own = (lax.ppermute(own, 'cp', [(0, 1)]), own)
            query = make_query()
            out, stat_own = attn_forward(local, scale, meta_own, 2, query, win_own)
            sh_blk = lax.dynamic_slice_in_dim(jnp.concatenate([shared, other, shared], axis=1), half * par, block, 1)
            win_sh = (lax.ppermute(sh_blk, 'cp', [(0, 1)]), sh_blk)
            out, stat_sh = attn_forward(local, scale, meta_sh, 1, query, win_sh, (out,))
            return out, (query, win_own, win_sh, stat_own, stat_sh)

        def attention_back(local, saved, grad_out, tau):
            query, win_own, win_sh, stat_own, stat_sh = saved
            grad_q, dprev, dcur = attn_backward(local, scale, meta_sh, 1, query, win_sh, stat_sh, grad_out, tau)
            sh_blk = dcur + lax.ppermute(dprev, 'cp', [(1, 0)]).astype(F32)
            mine = lax.dynamic_slice_in_dim(sh_blk, half * par, half, 1)
            theirs = lax.dynamic_slice_in_dim(sh_blk, half * (1 - par), half, 1).astype(BF16)
            theirs = swap(theirs)
            grad_q, dprev, dcur = attn_backward(local, scale, meta_own, 2, query, win_own, stat_own, grad_out, tau,
                                                (grad_q,))
            mine = (mine + theirs.astype(F32)).astype(BF16)
            own = (dcur + lax.ppermute(dprev, 'cp', [(1, 0)]).astype(F32)).astype(BF16)
            long = jnp.concatenate([mine, own, mine], axis=1)
            return grad_q, lax.dynamic_slice_in_dim(long, half * (1 - par), n_rows, 1)

        def exchange(pick, place, buf):
            for k in range(tp_size):
                peer = tp_rank ^ k
                piece = pick(peer)
                if k:
                    piece = lax.ppermute(piece, 'tp', [(i, i ^ k) for i in range(tp_size)])
                buf = place(buf, piece, peer)
            return buf

        def to_groups(val):
            return exchange(lambda p: lax.dynamic_index_in_dim(val, p, 0, keepdims=False),
                            lambda buf, piece, p: lax.dynamic_update_slice_in_dim(buf, piece, p * n_rows, 0),
                            jnp.zeros((batch * block, val.shape[2]), val.dtype))

        def heads_to_groups(val):
            return exchange(lambda p: lax.dynamic_slice_in_dim(val, p * head_dim, head_dim, 2),
                            lambda buf, piece, p: lax.dynamic_update_slice_in_dim(buf, piece, p * n_rows, 1),
                            jnp.zeros((2, batch * block, head_dim), val.dtype))

        def to_all(rows):
            return lax.all_gather(rows, 'tp', axis=0, tiled=True).reshape(batch, block, d_model)

        def to_all_early(rows):
            parts = jnp.stack([cols(rows, 0), cols(rows, 1)])
            parts = lax.all_gather(parts, 'tp', axis=0, tiled=False)
            pieces = [parts[:, side].reshape(batch, block, d_model // 2) for side in range(2)]
            return jnp.concatenate(pieces, axis=2)

        def cp_sum(part_of):
            sent = lax.ppermute(part_of(1 - cp_rank), 'cp', [(0, 1), (1, 0)])
            return part_of(cp_rank) + sent

        def cols(val, half_no):
            return lax.dynamic_slice_in_dim(val, half_no * (d_model // 2), d_model // 2, 1)

        def head_rows(val, half_no):
            return lax.dynamic_index_in_dim(val, half_no, 0, keepdims=False)

        w_qkv_a = gather_qkv(wq_a, wk_a, wv_a)
        w_out_a = gather_out(wo_a)
        w_qkv_b = gather_qkv(wq_b, wk_b, wv_b)
        w_out_b = gather_out(wo_b)

        key_at = [block * (1 - cp_rank), positions[0] - block]
        meta_own = jnp.stack([par, block + 0 * par] + key_at).astype(jnp.int32)
        meta_sh = jnp.stack([2 * (1 - par), block + half * par] + key_at).astype(jnp.int32)
        cos_r = row_table(rope_cos)
        sin_r = row_table(rope_sin)
        q_temp = row_table(value_a11(positions))
        ones = jnp.ones((1, n_rows), F32)

        xn_all = rms_norm(x_in, norm_a).reshape(batch * block, d_model)
        xn_a = lax.dynamic_slice_in_dim(xn_all, tp_rank * n_rows, n_rows, 0)
        x_rows = my_rows(x_in)
        gy_rows = my_rows(grad_y)
        kv_raw = dot_f32('rd,tdh->trh', xn_a, w_qkv_a[1]).astype(BF16)
        kv_a = prep_call(prep_kernel, 1, kv_raw, cos_r, sin_r)

        def query_a():
            raw = dot_f32('rd,tdh->trh', xn_a, w_qkv_a[0]).astype(BF16)
            q_raws.append(raw)
            return prep_call(prep_kernel, 2, raw, cos_r, sin_r)

        q_raws = []
        out_a, saved_a = attention(True, kv_a, query_a)
        q_raw = q_raws[0]
        attn_a = dot_f32('crh,chd->rd', out_a, w_out_a).astype(BF16)
        h_rows = (x_rows.astype(F32) + attn_a.astype(F32)).astype(BF16)

        xn_b = rms_norm(h_rows, norm_b)
        kv_b = dot_f32('rd,tdh->trh', xn_b, w_qkv_b[1]).astype(BF16)

        def query_b():
            raw = dot_f32('rd,tdh->trh', xn_b, w_qkv_b[0]).astype(BF16)
            return (raw.astype(F32) * q_temp[None, :, None]).astype(BF16)

        out_b, saved_b = attention(False, kv_b, query_b)
        attn_b = dot_f32('crh,chd->rd', out_b, w_out_b).astype(BF16)
        y_rows = (h_rows.astype(F32) + attn_b.astype(F32)).astype(BF16)
        out_y = to_all_early(y_rows)
        gy_rows, _ = lax.optimization_barrier((gy_rows, y_rows))

        grad_ob = dot_f32('rd,chd->crh', gy_rows, w_out_b).astype(BF16)
        grad_q_b, grad_kv_b = attention_back(False, saved_b, grad_ob, q_temp[None, :])
        out_b_group = heads_to_groups(out_b)
        gy_all = grad_y.reshape(batch * block, d_model)
        grad_wo_b = cp_sum(lambda half_no: dot_f32('rh,rd->hd', head_rows(out_b_group, half_no), gy_all))
        parts = []
        for grad_part in (grad_q_b, grad_kv_b):
            part_b = cp_sum(lambda half_no: dot_f32('rd,trh->thd', cols(xn_b, half_no), grad_part))
            part_b = with_layout_constraint(part_b.reshape(-1, d_model // 2), Layout((0, 1)))
            part_b = lax.psum_scatter(part_b, 'tp', scatter_dimension=0, tiled=True)
            part_b = with_layout_constraint(part_b, Layout((0, 1)))
            parts.append(part_b.T)
        grad_wq_b, grad_wkv_b = parts
        grad_xn_b = (dot_f32('trh,tdh->rd', grad_q_b, w_qkv_b[0])
                     + dot_f32('trh,tdh->rd', grad_kv_b, w_qkv_b[1])).astype(BF16)
        grad_h_norm, gain_b = norm_backward(h_rows, norm_b, grad_xn_b.astype(F32))
        grad_h = (gy_rows.astype(F32) + grad_h_norm).astype(BF16)

        grad_oa = dot_f32('rd,chd->crh', grad_h, w_out_a).astype(BF16)
        grad_q_a, grad_kv_a = attention_back(True, saved_a, grad_oa, ones)
        part_o = cp_sum(lambda half_no: dot_f32('rh,rd->hd', head_rows(out_a, half_no), grad_h))
        grad_wo_a = lax.psum_scatter(part_o, 'tp', scatter_dimension=0, tiled=True)
        grad_q_raw = prep_call(prep_back_kernel, 2, q_raw, cos_r, sin_r, grad_q_a)
        grad_kv_raw = prep_call(prep_back_kernel, 1, kv_raw, cos_r, sin_r, grad_kv_a)
        grad_xn_q = dot_f32('trh,tdh->rd', grad_q_raw, w_qkv_a[0])
        grad_xn_a = (grad_xn_q + dot_f32('trh,tdh->rd', grad_kv_raw, w_qkv_a[1])).astype(BF16)
        grad_x_norm, gain_a = norm_backward(x_rows, norm_a, grad_xn_a.astype(F32))
        gx_rows = (grad_h.astype(F32) + grad_x_norm).astype(BF16)
        grad_x = to_all(gx_rows)
        grad_q_group = to_groups(grad_q_raw)
        grad_kv_group = to_groups(grad_kv_raw)
        grad_wq_a = cp_sum(lambda half_no: dot_f32('rd,rh->dh', cols(xn_all, half_no), grad_q_group))
        grad_wkv_a = cp_sum(lambda half_no: dot_f32('rd,rh->dh', cols(xn_all, half_no), grad_kv_group))

        gains = lax.psum(jnp.stack([gain_a, gain_b]), ('tp', 'cp'))
        gains = lax.dynamic_slice_in_dim(gains, cp_rank * (d_model // 2), d_model // 2, 1).astype(BF16)
        grad_wo_b, grad_wo_a, grad_wq_a, grad_wkv_a, grad_wq_b, grad_wkv_b = (
            val.astype(BF16) for val in (grad_wo_b, grad_wo_a, grad_wq_a, grad_wkv_a, grad_wq_b, grad_wkv_b))
        return (out_y, grad_x,
                gains[0], grad_wq_a, grad_wkv_a[:, :head_dim], grad_wkv_a[:, head_dim:], grad_wo_a,
                gains[1], grad_wq_b, grad_wkv_b[:, :head_dim], grad_wkv_b[:, head_dim:], grad_wo_b)

    return jax.shard_map(body, mesh=mesh, in_specs=in_specs, out_specs=out_specs, check_vma=False)
```
